32 devices in a mesh: dp: 16 (over z, y, x), mp: 2 (over core).
Axes of the slice: x: 2, y: 2, z: 4, core: 2. Of those that a mesh axis runs over, the one named last changes fastest.
Arguments:
- pooled_grad: bfloat16 [4096, 32, 128], P(('dp', 'mp')), may hold values from -6 to 6
- bag_lengths: int32 [4096, 32], P(('dp', 'mp')), may hold values from 1 to 4
- bag_rows: int32 [4096, 32, 4], P(('dp', 'mp')), may hold values from 0 to 2047
- table_rows: float32 [32, 2048, 128], P('dp', 'mp'), may hold values from -6 to 6
- row_accum: float32 [32, 2048], P('dp', 'mp'), may hold values from 0.01 to 1
- dense_input: bfloat16 [4096, 1024], P(('dp', 'mp')), may hold values from -6 to 6
- dense_cotangent: bfloat16 [4096, 1024], P(('dp', 'mp')), may hold values from -0.09375 to 0.09375
Outputs:
- new_rows: float32 [32, 2048, 128], P('dp', 'mp')
- new_accum: float32 [32, 2048], P('dp', 'mp')
- dense_grad: float32 [1024, 1024], replicated
The draws below stay inside these ranges and needn't reach their ends.
Inputs may be any that keep to these rules, and one draw needn't show every extreme that they name: `bag_rows`: a row number of the whole table.
All inputs are finite; a program needn't handle non-finite values.
Results may differ from the reference program's by a relative error of at most 0.0003.
Values may be sent and summed in bfloat16 or wider, within the bound.
A program may use at most 128 MiB of HBM per device.

```python
import math
import jax
import jax.numpy as jnp
import numpy as np
from jax import lax

E = 128
D_IN = 1024
D_OUT = 1024
BAG = 4
TABLES = 32
ROWS = 2048
B_ALL = 4096


def plant(drawn, own_key, smallest, top_value):
    index_at = [jax.random.randint(jax.random.fold_in(own_key, axis), (), 0, length) for axis, length in enumerate(drawn.shape)]
    widest = drawn.shape.index(max(drawn.shape))
    beside = index_at[:widest] + [(index_at[widest] + 1) % drawn.shape[widest]] + index_at[widest + 1:]
    return drawn.at[tuple(index_at)].set(smallest).at[tuple(beside)].set(top_value)


def block_scale(own_key, shape, split, least, high):
    gain, own = 1.0, jax.random.fold_in(own_key, 6)
    for position, parts in split:
        draws = jnp.exp(jax.random.uniform(jax.random.fold_in(own, position), (parts,), jnp.float32, least / len(split), high / len(split)))
        gain = gain * jnp.repeat(draws, shape[position] // parts).reshape([-1 if axis == position else 1 for axis in range(len(shape))])
    return gain


def rank_table(number_of, skew):
    loads = [(1 << 20) // math.isqrt(standing ** skew) + 1 for standing in range(1, number_of + 1)]
    scale = 1 + sum(loads) // (1 << 30)
    return np.cumsum(np.array([max(1, weight // scale) for weight in loads]))


def ranked_ids(own_key, dims, amount, skew):
    table = rank_table(amount, skew)
    ticket = jax.random.randint(jax.random.fold_in(own_key, 1), dims, 0, int(table[amount - 1]))
    rank = jnp.searchsorted(jnp.asarray(table, jnp.int32), ticket, side="right")
    return jax.random.permutation(jax.random.fold_in(own_key, 2), amount)[rank].astype(jnp.int32)


def noise(key, dims, deviation, reach, split=(), kind=jnp.bfloat16):
    gain = block_scale(key, dims, split, -0.22, 0.18) if split else 1.0
    result = jax.random.normal(key, dims, jnp.float32) * deviation * gain
    return jnp.minimum(jnp.maximum(result, -reach), reach).astype(kind)


def setup_inputs(seed: int = 0) -> dict:
    keys = jax.random.split(jax.random.key(seed), 8)
    pooled_grad = noise(keys[0], (B_ALL, TABLES, E), 1.0, 6.0, ((0, 32),))
    bag_lengths = plant(jax.random.randint(keys[1], (B_ALL, TABLES), 1, BAG + 1), jax.random.fold_in(keys[1], 1), 1, BAG).astype(jnp.int32)
    bag_rows = plant(ranked_ids(keys[2], (B_ALL, TABLES, BAG), ROWS, 2), jax.random.fold_in(keys[2], 3), 0, ROWS - 1).astype(jnp.int32)
    table_rows = noise(keys[3], (TABLES, ROWS, E), 1.0, 6.0, ((0, 16), (1, 2)), jnp.float32)
    row_accum = jnp.clip(jnp.exp(math.log(1.0) - 4.6051702 * jax.random.uniform(keys[4], (TABLES, ROWS), jnp.float32) ** block_scale(keys[4], (TABLES, ROWS), ((0, 16), (1, 2)), -0.2, 0.2)), 0.01, 1.0)
    dense_input = noise(keys[5], (B_ALL, D_IN), 1.0, 6.0, ((0, 32),))
    dense_cotangent = noise(keys[6], (B_ALL, D_OUT), B_ALL ** -0.5, 0.09375, ((0, 32),))
    return dict(pooled_grad=pooled_grad, bag_lengths=bag_lengths, bag_rows=bag_rows, table_rows=table_rows, row_accum=row_accum, dense_input=dense_input, dense_cotangent=dense_cotangent)


learn_rate = 0.5

def reference(pooled_grad, bag_lengths, bag_rows, table_rows, row_accum, dense_input, dense_cotangent):

    def one_table(table):
        column_grad = lax.dynamic_index_in_dim(pooled_grad, table, 1, keepdims=False)
        lengths = lax.dynamic_index_in_dim(bag_lengths, table, 1, keepdims=False)
        looked = lax.dynamic_index_in_dim(bag_rows, table, 1, keepdims=False)
        active = jnp.arange(BAG, dtype=jnp.int32)[None, :] < lengths[:, None]
        values = jnp.where(active[..., None], column_grad[:, None, :].astype(jnp.float32), jnp.zeros((), jnp.float32))
        values = values.reshape(-1, column_grad.shape[-1])
        return jax.ops.segment_sum(values, looked.reshape(-1).astype(jnp.int32), num_segments=ROWS)
    row_grad = lax.map(one_table, jnp.arange(TABLES, dtype=jnp.int32))
    new_accum = row_accum + lax.optimization_barrier(jnp.mean(row_grad * row_grad, axis=-1))
    new_rows = table_rows - learn_rate * row_grad / jnp.sqrt(new_accum)[..., None]
    dense_grad = lax.dot_general(dense_input, dense_cotangent, (((0,), (0,)), ((), ())), preferred_element_type=jnp.float32)
    return (new_rows, new_accum, dense_grad)
```

```python
import functools

import jax
import jax.numpy as jnp
from jax import lax
from jax.experimental import pallas as pl
from jax.experimental.pallas import tpu as pltpu
from jax.sharding import PartitionSpec as P

learn_rate = 0.5
MESH = pl.DeviceIdType.MESH


def loop(count, body):
    def step(k, carry):
        body(k)
        return carry

    lax.fori_loop(0, count, step, 0)


def exchange_kernel(
    dp, mp, inner, row_parts,
    g_ref, i_ref, din_ref, dcot_ref,
    gbuf, ibuf, dense,
    abuf, bbuf, part, rbuf,
    a_send, a_recv, b_send, b_recv, g_send, g_recv, i_send, i_recv,
    gf_send, gf_recv, if_send, if_recv,
    r_send, r_recv, z_send, z_recv, x_send, x_recv, m_send, m_recv,
):
    me = lax.axis_index("dp")
    m = lax.axis_index("mp")
    outer = dp // inner
    z, i = me // inner, me % inner
    group = inner * mp
    col_parts = group // row_parts
    rows, cols = dense.shape[0] // row_parts, dense.shape[1] // col_parts
    piece = rows // outer
    mine = i * mp + m

    barrier = pltpu.get_barrier_semaphore()

    def signal(d, q):
        pl.semaphore_signal(barrier, inc=1, device_id=(d, q), device_id_type=MESH)

    loop(dp - 1, lambda k: signal((me + 1 + k) % dp, m))
    loop((mp - 1) * inner, lambda k: signal(z * inner + k % inner, (m + 1 + k // inner) % mp))
    pl.semaphore_wait(barrier, dp - 1 + (mp - 1) * inner)

    def remote(src, dst, send, recv, d, q):
        return pltpu.make_async_remote_copy(
            src_ref=src, dst_ref=dst, send_sem=send, recv_sem=recv, device_id=(d, q), device_id_type=MESH
        )

    def row_span(p):
        return pl.ds(pl.multiple_of((p // col_parts) * rows, 128), rows)

    def col_span(p):
        return pl.ds(pl.multiple_of((p % col_parts) * cols, 128), cols)

    def a_copy(k):
        p = (mine + 1 + k) % group
        return remote(din_ref.at[:, row_span(p)], abuf.at[mine], a_send.at[k], a_recv.at[mine], z * inner + p // mp, p % mp)

    def b_copy(k):
        p = (mine + 1 + k) % group
        return remote(dcot_ref.at[:, col_span(p)], bbuf.at[mine], b_send.at[k], b_recv.at[mine], z * inner + p // mp, p % mp)

    def start_dense(k):
        a_copy(k).start()
        b_copy(k).start()

    loop(group - 1, start_dense)

    def g_copy(k):
        d = (me + 1 + k) % dp
        return remote(g_ref.at[d], gbuf.at[me, m], g_send.at[k], g_recv.at[me], d, m)

    def i_copy(k):
        d = (me + 1 + k) % dp
        return remote(i_ref.at[d], ibuf.at[me, m], i_send.at[k], i_recv.at[me], d, m)

    def start_grads(k):
        g_copy(k).start()
        i_copy(k).start()

    loop(dp - 1, start_grads)

    def forward(s, k, src_g, src_i):
        q = (m + 1 + k) % mp
        return (
            remote(src_g, gbuf.at[s, m], gf_send.at[k, s], gf_recv.at[m, s], me, q),
            remote(src_i, ibuf.at[s, m], if_send.at[k, s], if_recv.at[m, s], me, q),
        )

    def start_forward(s, src_g, src_i):
        for k in range(mp - 1):
            for copy in forward(s, k, src_g, src_i):
                copy.start()

    start_forward(me, g_ref.at[me], i_ref.at[me])
    gbuf[me, m] = g_ref[me]
    ibuf[me, m] = i_ref[me]
    abuf[mine] = din_ref[:, row_span(mine)]
    bbuf[mine] = dcot_ref[:, col_span(mine)]

    def wait_dense(k):
        s = (mine + 1 + k) % group
        remote(abuf.at[s], abuf.at[s], a_send.at[k], a_recv.at[s], me, m).wait_recv()
        remote(bbuf.at[s], bbuf.at[s], b_send.at[k], b_recv.at[s], me, m).wait_recv()

    loop(group - 1, wait_dense)
    depth = abuf.shape[0] * abuf.shape[1]
    part[...] = lax.dot_general(
        abuf[...].reshape(depth, rows), bbuf[...].reshape(depth, cols), (((0,), (0,)), ((), ())),
        preferred_element_type=jnp.float32,
    )

    def piece_of(ref, w):
        return ref.at[pl.ds(pl.multiple_of(w * piece, 8), piece)]

    def r_copy(k):
        w = (z + 1 + k) % outer
        return remote(piece_of(part, w), rbuf.at[z], r_send.at[k], r_recv.at[z], w * inner + i, m)

    loop(outer - 1, lambda k: r_copy(k).start())
    own = part[pl.ds(pl.multiple_of(z * piece, 8), piece)]

    def spot(j, q, w):
        p = j * mp + q
        top = pl.multiple_of((p // col_parts) * rows + w * piece, 8)
        return pl.ds(top, piece), col_span(p)

    def at(j, q, w):
        return dense.at[spot(j, q, w)]

    rbuf[z] = own

    def wait_sum(k):
        s = (z + 1 + k) % outer
        remote(rbuf.at[s], rbuf.at[s], r_send.at[k], r_recv.at[s], me, m).wait_recv()

    loop(outer - 1, wait_sum)
    total = rbuf[0]
    for w in range(1, outer):
        total = total + rbuf[w]
    dense[spot(i, m, z)] = total

    def z_copy(k):
        w = (z + 1 + k) % outer
        return remote(at(i, m, z), at(i, m, z), z_send.at[k], z_recv.at[z], w * inner + i, m)

    def x_copy(k, w):
        j = (i + 1 + k) % inner
        return remote(at(i, m, w), at(i, m, w), x_send.at[k, w], x_recv.at[i, w], z * inner + j, m)

    def m_copy(k, j, w):
        return remote(at(j, m, w), at(j, m, w), m_send.at[k, j, w], m_recv.at[m, j, w], me, (m + 1 + k) % mp)

    def spread(w):
        loop(inner - 1, lambda k: x_copy(k, w).start())
        for k in range(mp - 1):
            m_copy(k, i, w).start()

    loop(outer - 1, lambda k: z_copy(k).start())
    spread(z)

    def pass_grads(k):
        s = (me + dp - 1 - k) % dp
        remote(gbuf.at[s, m], gbuf.at[s, m], g_send.at[k], g_recv.at[s], me, m).wait_recv()
        remote(ibuf.at[s, m], ibuf.at[s, m], i_send.at[k], i_recv.at[s], me, m).wait_recv()
        start_forward(s, gbuf.at[s, m], ibuf.at[s, m])

    def pass_piece(k):
        w = (z + 1 + k) % outer
        remote(at(i, m, w), at(i, m, w), z_send.at[k], z_recv.at[w], me, m).wait_recv()
        spread(w)

    loop(dp - 1, pass_grads)
    loop(outer - 1, pass_piece)

    def pass_block(t):
        k, w = t % (inner - 1), (z + t // (inner - 1)) % outer
        j = (i + 1 + k) % inner
        remote(at(j, m, w), at(j, m, w), x_send.at[k, w], x_recv.at[j, w], me, m).wait_recv()
        for n in range(mp - 1):
            m_copy(n, j, w).start()

    loop((inner - 1) * outer, pass_block)

    def end_forward(s):
        for k in range(mp - 1):
            q = (m + 1 + k) % mp
            remote(gbuf.at[s, q], gbuf.at[s, q], gf_send.at[k, s], gf_recv.at[q, s], me, m).wait_recv()
            remote(ibuf.at[s, q], ibuf.at[s, q], if_send.at[k, s], if_recv.at[q, s], me, m).wait_recv()
            for copy in forward(s, k, gbuf.at[s, m], ibuf.at[s, m]):
                copy.wait_send()

    loop(dp, end_forward)

    def end_block(t):
        j, w = t // outer, t % outer
        for k in range(mp - 1):
            q = (m + 1 + k) % mp
            remote(at(j, q, w), at(j, q, w), m_send.at[k, j, w], m_recv.at[q, j, w], me, m).wait_recv()
            m_copy(k, j, w).wait_send()

    loop(inner * outer, end_block)

    def end_dense(k):
        a_copy(k).wait_send()
        b_copy(k).wait_send()

    def end_grads(k):
        g_copy(k).wait_send()
        i_copy(k).wait_send()

    loop(group - 1, end_dense)
    loop(dp - 1, end_grads)

    def end_sum(k):
        r_copy(k).wait_send()
        z_copy(k).wait_send()

    loop(outer - 1, end_sum)
    loop((inner - 1) * outer, lambda t: x_copy(t % (inner - 1), t // (inner - 1)).wait_send())


def rows_kernel(slots, chunk, g_ref, i_ref, out_ref):
    tables, row_count = out_ref.shape[0], out_ref.shape[1]
    samples = i_ref.shape[2]
    base = lax.axis_index("mp") * row_count
    row_iota = lax.broadcasted_iota(jnp.int32, (row_count, samples), 0) + base
    out_ref[...] = jnp.zeros_like(out_ref)

    def add(c):
        for t in range(tables):
            hots = []
            for u in range(chunk):
                wanted = i_ref[c * chunk + u]
                hot = jnp.zeros((row_count, samples), jnp.float32)
                for s in range(slots):
                    one = wanted[t * slots + s : t * slots + s + 1, :]
                    hot = hot + jnp.where(row_iota == one, 1.0, 0.0)
                hots.append(hot.astype(jnp.bfloat16))
            onehot = jnp.concatenate(hots, axis=1)
            values = g_ref[pl.ds(c * chunk, chunk), t].reshape(chunk * samples, g_ref.shape[3])
            out_ref[t] += jnp.dot(onehot, values, preferred_element_type=jnp.float32)

    loop(i_ref.shape[0] // chunk, add)


def per_device(dp, mp, pooled_grad, bag_lengths, bag_rows, table_rows, row_accum, dense_input, dense_cotangent):
    samples, all_tables, width = pooled_grad.shape
    slots = bag_rows.shape[2]
    tables, row_count = table_rows.shape[0], table_rows.shape[1]
    inner = 4 if dp % 4 == 0 else 1
    outer = dp // inner
    group = inner * mp
    row_parts = 2 if group % 2 == 0 else 1
    in_width, out_width = dense_input.shape[1], dense_cotangent.shape[1]
    rows, cols = in_width // row_parts, out_width // (group // row_parts)

    slot_iota = jnp.arange(slots, dtype=jnp.int32)
    target = jnp.where(slot_iota[None, None, :] < bag_lengths[..., None], bag_rows, -1)
    target = target.transpose(1, 2, 0).reshape(dp, tables * slots, samples)
    grads = pooled_grad.transpose(1, 0, 2).reshape(dp, tables, samples, width)

    vmem = pl.BlockSpec(memory_space=pltpu.VMEM)
    dma = pltpu.SemaphoreType.DMA
    pairs = max(1, mp - 1)
    gathered, targets, dense_grad = pl.pallas_call(
        functools.partial(exchange_kernel, dp, mp, inner, row_parts),
        out_shape=(
            jax.ShapeDtypeStruct((dp, mp, tables, samples, width), jnp.bfloat16),
            jax.ShapeDtypeStruct((dp, mp, tables * slots, samples), jnp.int32),
            jax.ShapeDtypeStruct((in_width, out_width), jnp.float32),
        ),
        in_specs=[vmem] * 4,
        out_specs=(vmem,) * 3,
        scratch_shapes=[
            pltpu.VMEM((group, samples, rows), jnp.bfloat16),
            pltpu.VMEM((group, samples, cols), jnp.bfloat16),
            pltpu.VMEM((rows, cols), jnp.float32),
            pltpu.VMEM((outer, rows // outer, cols), jnp.float32),
            dma((group,)), dma((group,)), dma((group,)), dma((group,)),
            dma((dp,)), dma((dp,)), dma((dp,)), dma((dp,)),
            dma((pairs, dp)), dma((mp, dp)), dma((pairs, dp)), dma((mp, dp)),
            dma((outer,)), dma((outer,)), dma((outer,)), dma((outer,)),
            dma((inner, outer)), dma((inner, outer)),
            dma((pairs, inner, outer)), dma((mp, inner, outer)),
        ],
        compiler_params=pltpu.CompilerParams(collective_id=0, has_side_effects=True),
        name="exchange",
    )(grads, target, dense_input, dense_cotangent)

    sources = dp * mp
    row_grad = pl.pallas_call(
        functools.partial(rows_kernel, slots, 2 if sources % 2 == 0 else 1),
        out_shape=jax.ShapeDtypeStruct((tables, row_count, width), jnp.float32),
        in_specs=[vmem] * 2,
        out_specs=vmem,
        name="rows",
    )(gathered.reshape(sources, tables, samples, width), targets.reshape(sources, tables * slots, samples))

    new_accum = row_accum + jnp.mean(row_grad * row_grad, axis=-1)
    new_rows = table_rows - learn_rate * row_grad / jnp.sqrt(new_accum)[..., None]
    return (new_rows, new_accum, dense_grad)


def solution(mesh):
    in_specs = (
        P(("dp", "mp"), None, None),
        P(("dp", "mp"), None),
        P(("dp", "mp"), None, None),
        P("dp", "mp", None),
        P("dp", "mp"),
        P(("dp", "mp"), None),
        P(("dp", "mp"), None),
    )
    out_specs = (P("dp", "mp", None), P("dp", "mp"), P())
    body = functools.partial(per_device, mesh.shape["dp"], mesh.shape["mp"])
    return jax.shard_map(body, mesh=mesh, in_specs=in_specs, out_specs=out_specs, check_vma=False)
```

```python
import functools

import jax
import jax.numpy as jnp
from jax import lax
from jax.experimental import pallas as pl
from jax.experimental.pallas import tpu as pltpu
from jax.sharding import PartitionSpec as P

learn_rate = 0.5
MESH = pl.DeviceIdType.MESH


def loop(count, body):
    def step(k, carry):
        body(k)
        return carry

    lax.fori_loop(0, count, step, 0)


def exchange_kernel(
    dp, mp, inner, row_parts, slots,
    g_ref, i_ref, din_ref, dcot_ref,
    dense, row_grad,
    gbuf, ibuf, abuf, bbuf, part, rbuf,
    a_send, a_recv, af_send, af_recv, b_send, b_recv, g_send, g_recv, i_send, i_recv,
    gf_send, gf_recv, if_send, if_recv,
    r_send, r_recv, z_send, z_recv, x_send, x_recv, m_send, m_recv,
):
    me = lax.axis_index("dp")
    m = lax.axis_index("mp")
    outer = dp // inner
    z, i = me // inner, me % inner
    group = inner * mp
    col_parts = group // row_parts
    rows, cols = dense.shape[0] // row_parts, dense.shape[1] // col_parts
    piece = rows // outer
    mine = i * mp + m

    barrier = pltpu.get_barrier_semaphore()

    def signal(d, q):
        pl.semaphore_signal(barrier, inc=1, device_id=(d, q), device_id_type=MESH)

    loop(dp - 1, lambda k: signal((me + 1 + k) % dp, m))
    loop((mp - 1) * inner, lambda k: signal(z * inner + k % inner, (m + 1 + k // inner) % mp))
    pl.semaphore_wait(barrier, dp - 1 + (mp - 1) * inner)

    def remote(src, dst, send, recv, d, q):
        return pltpu.make_async_remote_copy(
            src_ref=src, dst_ref=dst, send_sem=send, recv_sem=recv, device_id=(d, q), device_id_type=MESH
        )

    def row_span(p):
        return pl.ds(pl.multiple_of((p // col_parts) * rows, 128), rows)

    def col_span(p):
        return pl.ds(pl.multiple_of((p % col_parts) * cols, 128), cols)

    def a_copy(k):
        j = (i + 1 + k) % inner
        return remote(din_ref.at[:, row_span(j * mp)], abuf.at[mine], a_send.at[k], a_recv.at[i], z * inner + j, m)

    def a_pass(k, j, src):
        return remote(src, abuf.at[j * mp + m], af_send.at[k, j], af_recv.at[m, j], me, (m + 1 + k) % mp)

    def b_copy(k):
        p = (mine + 1 + k) % group
        return remote(dcot_ref.at[:, col_span(p)], bbuf.at[mine], b_send.at[k], b_recv.at[mine], z * inner + p // mp, p % mp)

    loop(inner - 1, lambda k: a_copy(k).start())
    loop(group - 1, lambda k: b_copy(k).start())
    for k in range(mp - 1):
        a_pass(k, i, din_ref.at[:, row_span(mine)]).start()

    def g_copy(k):
        d = (me + 1 + k) % dp
        return remote(g_ref.at[d], gbuf.at[me, m], g_send.at[k], g_recv.at[me], d, m)

    def i_copy(k):
        d = (me + 1 + k) % dp
        return remote(i_ref.at[d], ibuf.at[me, m], i_send.at[k], i_recv.at[me], d, m)

    def start_grads(k):
        g_copy(k).start()
        i_copy(k).start()

    loop(dp - 1, start_grads)

    def forward(s, k, src_g, src_i):
        q = (m + 1 + k) % mp
        return (
            remote(src_g, gbuf.at[s, m], gf_send.at[k, s], gf_recv.at[m, s], me, q),
            remote(src_i, ibuf.at[s, m], if_send.at[k, s], if_recv.at[m, s], me, q),
        )

    def start_forward(s, src_g, src_i):
        for k in range(mp - 1):
            for copy in forward(s, k, src_g, src_i):
                copy.start()

    start_forward(me, g_ref.at[me], i_ref.at[me])
    gbuf[me, m] = g_ref[me]
    ibuf[me, m] = i_ref[me]
    abuf[mine] = din_ref[:, row_span(mine)]
    bbuf[mine] = dcot_ref[:, col_span(mine)]

    row_grad[...] = jnp.zeros_like(row_grad)

    def pass_a(k):
        j = (i + inner - 1 - k) % inner
        s = j * mp + m
        remote(abuf.at[s], abuf.at[s], a_send.at[k], a_recv.at[j], me, m).wait_recv()
        for n in range(mp - 1):
            a_pass(n, j, abuf.at[s]).start()

    loop(inner - 1, pass_a)

    def wait_a(j):
        for k in range(mp - 1):
            q = (m + 1 + k) % mp
            s = j * mp + q
            remote(abuf.at[s], abuf.at[s], af_send.at[k, j], af_recv.at[q, j], me, m).wait_recv()

    def wait_b(k):
        s = (mine + 1 + k) % group
        remote(bbuf.at[s], bbuf.at[s], b_send.at[k], b_recv.at[s], me, m).wait_recv()

    loop(group - 1, wait_b)
    loop(inner, wait_a)
    depth = abuf.shape[0] * abuf.shape[1]
    part[...] = lax.dot_general(
        abuf[...].reshape(depth, rows), bbuf[...].reshape(depth, cols), (((0,), (0,)), ((), ())),
        preferred_element_type=jnp.float32,
    )

    def piece_of(ref, w):
        return ref.at[pl.ds(pl.multiple_of(w * piece, 8), piece)]

    def r_copy(k):
        w = (z + 1 + k) % outer
        return remote(piece_of(part, w), rbuf.at[z], r_send.at[k], r_recv.at[z], w * inner + i, m)

    loop(outer - 1, lambda k: r_copy(k).start())
    own = part[pl.ds(pl.multiple_of(z * piece, 8), piece)]

    def spot(j, q, w):
        p = j * mp + q
        top = pl.multiple_of((p // col_parts) * rows + w * piece, 8)
        return pl.ds(top, piece), col_span(p)

    def at(j, q, w):
        return dense.at[spot(j, q, w)]

    rbuf[z] = own

    def pass_grads(k):
        s = (me + dp - 1 - k) % dp
        remote(gbuf.at[s, m], gbuf.at[s, m], g_send.at[k], g_recv.at[s], me, m).wait_recv()
        remote(ibuf.at[s, m], ibuf.at[s, m], i_send.at[k], i_recv.at[s], me, m).wait_recv()
        start_forward(s, gbuf.at[s, m], ibuf.at[s, m])

    loop(dp - 1, pass_grads)

    tables, row_count, width = row_grad.shape
    samples = i_ref.shape[2]
    row_iota = lax.broadcasted_iota(jnp.int32, (row_count, samples), 0) + m * row_count

    def add_source(c):
        s = (me + dp - c) % dp
        for k in range(mp - 1):
            q = (m + 1 + k) % mp
            remote(gbuf.at[s, q], gbuf.at[s, q], gf_send.at[k, s], gf_recv.at[q, s], me, m).wait_recv()
            remote(ibuf.at[s, q], ibuf.at[s, q], if_send.at[k, s], if_recv.at[q, s], me, m).wait_recv()
        for t in range(tables):
            hots = []
            for u in range(mp):
                wanted = ibuf[s, u]
                hot = jnp.zeros((row_count, samples), jnp.float32)
                for n in range(slots):
                    one = wanted[t * slots + n : t * slots + n + 1, :]
                    hot = hot + jnp.where(row_iota == one, 1.0, 0.0)
                hots.append(hot.astype(jnp.bfloat16))
            onehot = jnp.concatenate(hots, axis=1)
            values = gbuf[s, :, t].reshape(mp * samples, width)
            row_grad[t] += jnp.dot(onehot, values, preferred_element_type=jnp.float32)

    early = dp // 2
    loop(early, add_source)

    def wait_sum(k):
        s = (z + 1 + k) % outer
        remote(rbuf.at[s], rbuf.at[s], r_send.at[k], r_recv.at[s], me, m).wait_recv()

    loop(outer - 1, wait_sum)
    total = rbuf[0]
    for w in range(1, outer):
        total = total + rbuf[w]
    dense[spot(i, m, z)] = total

    def z_copy(k):
        w = (z + 1 + k) % outer
        return remote(at(i, m, z), at(i, m, z), z_send.at[k], z_recv.at[z], w * inner + i, m)

    def x_copy(k, w):
        j = (i + 1 + k) % inner
        return remote(at(i, m, w), at(i, m, w), x_send.at[k, w], x_recv.at[i, w], z * inner + j, m)

    def m_copy(k, j, w):
        return remote(at(j, m, w), at(j, m, w), m_send.at[k, j, w], m_recv.at[m, j, w], me, (m + 1 + k) % mp)

    def spread(w):
        loop(inner - 1, lambda k: x_copy(k, w).start())
        for k in range(mp - 1):
            m_copy(k, i, w).start()

    loop(outer - 1, lambda k: z_copy(k).start())
    spread(z)

    def pass_piece(k):
        w = (z + 1 + k) % outer
        remote(at(i, m, w), at(i, m, w), z_send.at[k], z_recv.at[w], me, m).wait_recv()
        spread(w)

    loop(dp - early, lambda c: add_source(early + c))
    loop(outer - 1, pass_piece)

    def pass_block(t):
        k, w = t % (inner - 1), (z + t // (inner - 1)) % outer
        j = (i + 1 + k) % inner
        remote(at(j, m, w), at(j, m, w), x_send.at[k, w], x_recv.at[j, w], me, m).wait_recv()
        for n in range(mp - 1):
            m_copy(n, j, w).start()

    loop((inner - 1) * outer, pass_block)

    def end_forward(s):
        for k in range(mp - 1):
            for copy in forward(s, k, gbuf.at[s, m], ibuf.at[s, m]):
                copy.wait_send()

    loop(dp, end_forward)

    def end_block(t):
        j, w = t // outer, t % outer
        for k in range(mp - 1):
            q = (m + 1 + k) % mp
            remote(at(j, q, w), at(j, q, w), m_send.at[k, j, w], m_recv.at[q, j, w], me, m).wait_recv()
            m_copy(k, j, w).wait_send()

    loop(inner * outer, end_block)

    def end_a(j):
        for k in range(mp - 1):
            a_pass(k, j, abuf.at[j * mp + m]).wait_send()

    def end_grads(k):
        g_copy(k).wait_send()
        i_copy(k).wait_send()

    loop(inner - 1, lambda k: a_copy(k).wait_send())
    loop(inner, end_a)
    loop(group - 1, lambda k: b_copy(k).wait_send())
    loop(dp - 1, end_grads)

    def end_sum(k):
        r_copy(k).wait_send()
        z_copy(k).wait_send()

    loop(outer - 1, end_sum)
    loop((inner - 1) * outer, lambda t: x_copy(t % (inner - 1), t // (inner - 1)).wait_send())


def per_device(dp, mp, pooled_grad, bag_lengths, bag_rows, table_rows, row_accum, dense_input, dense_cotangent):
    samples, all_tables, width = pooled_grad.shape
    slots = bag_rows.shape[2]
    tables, row_count = table_rows.shape[0], table_rows.shape[1]
    inner = 4 if dp % 4 == 0 else 1
    outer = dp // inner
    group = inner * mp
    row_parts = 2 if inner % 2 == 0 else 1
    in_width, out_width = dense_input.shape[1], dense_cotangent.shape[1]
    rows, cols = in_width // row_parts, out_width // (group // row_parts)

    slot_iota = jnp.arange(slots, dtype=jnp.int32)
    target = jnp.where(slot_iota[None, None, :] < bag_lengths[..., None], bag_rows, -1)
    target = target.transpose(1, 2, 0).reshape(dp, tables * slots, samples)
    grads = pooled_grad.transpose(1, 0, 2).reshape(dp, tables, samples, width)

    vmem = pl.BlockSpec(memory_space=pltpu.VMEM)
    dma = pltpu.SemaphoreType.DMA
    pairs = max(1, mp - 1)
    dense_grad, row_grad = pl.pallas_call(
        functools.partial(exchange_kernel, dp, mp, inner, row_parts, slots),
        out_shape=(
            jax.ShapeDtypeStruct((in_width, out_width), jnp.float32),
            jax.ShapeDtypeStruct((tables, row_count, width), jnp.float32),
        ),
        in_specs=[vmem] * 4,
        out_specs=(vmem,) * 2,
        scratch_shapes=[
            pltpu.VMEM((dp, mp, tables, samples, width), jnp.bfloat16),
            pltpu.VMEM((dp, mp, tables * slots, samples), jnp.int32),
            pltpu.VMEM((group, samples, rows), jnp.bfloat16),
            pltpu.VMEM((group, samples, cols), jnp.bfloat16),
            pltpu.VMEM((rows, cols), jnp.float32),
            pltpu.VMEM((outer, rows // outer, cols), jnp.float32),
            dma((inner,)), dma((inner,)), dma((pairs, inner)), dma((mp, inner)), dma((group,)), dma((group,)),
            dma((dp,)), dma((dp,)), dma((dp,)), dma((dp,)),
            dma((pairs, dp)), dma((mp, dp)), dma((pairs, dp)), dma((mp, dp)),
            dma((outer,)), dma((outer,)), dma((outer,)), dma((outer,)),
            dma((inner, outer)), dma((inner, outer)),
            dma((pairs, inner, outer)), dma((mp, inner, outer)),
        ],
        compiler_params=pltpu.CompilerParams(collective_id=0, has_side_effects=True),
        name="exchange",
    )(grads, target, dense_input, dense_cotangent)

    new_accum = row_accum + jnp.mean(row_grad * row_grad, axis=-1)
    new_rows = table_rows - learn_rate * row_grad / jnp.sqrt(new_accum)[..., None]
    return (new_rows, new_accum, dense_grad)


def solution(mesh):
    in_specs = (
        P(("dp", "mp"), None, None),
        P(("dp", "mp"), None),
        P(("dp", "mp"), None, None),
        P("dp", "mp", None),
        P("dp", "mp"),
        P(("dp", "mp"), None),
        P(("dp", "mp"), None),
    )
    out_specs = (P("dp", "mp", None), P("dp", "mp"), P())
    body = functools.partial(per_device, mesh.shape["dp"], mesh.shape["mp"])
    return jax.shard_map(body, mesh=mesh, in_specs=in_specs, out_specs=out_specs, check_vma=False)
```

```python
import functools

import jax
import jax.numpy as jnp
from jax import lax
from jax.experimental import pallas as pl
from jax.experimental.pallas import tpu as pltpu
from jax.sharding import PartitionSpec as P

learn_rate = 0.5
MESH = pl.DeviceIdType.MESH


def loop(count, body):
    def step(k, carry):
        body(k)
        return carry

    lax.fori_loop(0, count, step, 0)


def exchange_kernel(
    dp, mp, inner, row_parts, slots,
    g_ref, i_ref, din_ref, dcot_ref,
    dense, row_grad,
    gbuf, ibuf, abuf, bbuf, part, rbuf,
    a_send, a_recv, af_send, af_recv, b_send, b_recv, g_send, g_recv, i_send, i_recv,
    gf_send, gf_recv, if_send, if_recv,
    r_send, r_recv, z_send, z_recv, x_send, x_recv, y_send, y_recv, m_send, m_recv,
):
    me = lax.axis_index("dp")
    m = lax.axis_index("mp")
    outer = dp // inner
    z, i = me // inner, me % inner
    group = inner * mp
    col_parts = group // row_parts
    rows, cols = dense.shape[0] // row_parts, dense.shape[1] // col_parts
    piece = rows // outer
    mine = i * mp + m

    barrier = pltpu.get_barrier_semaphore()

    def signal(d, q):
        pl.semaphore_signal(barrier, inc=1, device_id=(d, q), device_id_type=MESH)

    loop(dp - 1, lambda k: signal((me + 1 + k) % dp, m))
    loop((mp - 1) * inner, lambda k: signal(z * inner + k % inner, (m + 1 + k // inner) % mp))
    pl.semaphore_wait(barrier, dp - 1 + (mp - 1) * inner)

    def remote(src, dst, send, recv, d, q):
        return pltpu.make_async_remote_copy(
            src_ref=src, dst_ref=dst, send_sem=send, recv_sem=recv, device_id=(d, q), device_id_type=MESH
        )

    def row_span(p):
        return pl.ds(pl.multiple_of((p // col_parts) * rows, 128), rows)

    def col_span(p):
        return pl.ds(pl.multiple_of((p % col_parts) * cols, 128), cols)

    def a_copy(k):
        j = (i + 1 + k) % inner
        return remote(din_ref.at[:, row_span(j * mp)], abuf.at[mine], a_send.at[k], a_recv.at[i], z * inner + j, m)

    def a_pass(k, j, src):
        return remote(src, abuf.at[j * mp + m], af_send.at[k, j], af_recv.at[m, j], me, (m + 1 + k) % mp)

    def b_copy(k):
        p = (mine + 1 + k) % group
        return remote(dcot_ref.at[:, col_span(p)], bbuf.at[mine], b_send.at[k], b_recv.at[mine], z * inner + p // mp, p % mp)

    loop(inner - 1, lambda k: a_copy(k).start())
    loop(group - 1, lambda k: b_copy(k).start())
    for k in range(mp - 1):
        a_pass(k, i, din_ref.at[:, row_span(mine)]).start()

    def g_copy(k):
        d = (me + 1 + k) % dp
        return remote(g_ref.at[d], gbuf.at[me, m], g_send.at[k], g_recv.at[me], d, m)

    def i_copy(k):
        d = (me + 1 + k) % dp
        return remote(i_ref.at[d], ibuf.at[me, m], i_send.at[k], i_recv.at[me], d, m)

    def start_grads(k):
        g_copy(k).start()
        i_copy(k).start()

    loop(dp - 1, start_grads)

    def forward(s, k, src_g, src_i):
        q = (m + 1 + k) % mp
        return (
            remote(src_g, gbuf.at[s, m], gf_send.at[k, s], gf_recv.at[m, s], me, q),
            remote(src_i, ibuf.at[s, m], if_send.at[k, s], if_recv.at[m, s], me, q),
        )

    def start_forward(s, src_g, src_i):
        for k in range(mp - 1):
            for copy in forward(s, k, src_g, src_i):
                copy.start()

    start_forward(me, g_ref.at[me], i_ref.at[me])
    gbuf[me, m] = g_ref[me]
    ibuf[me, m] = i_ref[me]
    abuf[mine] = din_ref[:, row_span(mine)]
    bbuf[mine] = dcot_ref[:, col_span(mine)]

    row_grad[...] = jnp.zeros_like(row_grad)

    def pass_a(k):
        j = (i + inner - 1 - k) % inner
        s = j * mp + m
        remote(abuf.at[s], abuf.at[s], a_send.at[k], a_recv.at[j], me, m).wait_recv()
        for n in range(mp - 1):
            a_pass(n, j, abuf.at[s]).start()

    loop(inner - 1, pass_a)

    def wait_a(j):
        for k in range(mp - 1):
            q = (m + 1 + k) % mp
            s = j * mp + q
            remote(abuf.at[s], abuf.at[s], af_send.at[k, j], af_recv.at[q, j], me, m).wait_recv()

    def wait_b(k):
        s = (mine + 1 + k) % group
        remote(bbuf.at[s], bbuf.at[s], b_send.at[k], b_recv.at[s], me, m).wait_recv()

    loop(group - 1, wait_b)
    loop(inner, wait_a)
    depth = abuf.shape[0] * abuf.shape[1]
    part[...] = lax.dot_general(
        abuf[...].reshape(depth, rows), bbuf[...].reshape(depth, cols), (((0,), (0,)), ((), ())),
        preferred_element_type=jnp.float32,
    )

    def piece_of(ref, w):
        return ref.at[pl.ds(pl.multiple_of(w * piece, 8), piece)]

    def r_copy(k):
        w = (z + 1 + k) % outer
        return remote(piece_of(part, w), rbuf.at[z], r_send.at[k], r_recv.at[z], w * inner + i, m)

    loop(outer - 1, lambda k: r_copy(k).start())
    own = part[pl.ds(pl.multiple_of(z * piece, 8), piece)]

    def spot(j, q, w):
        p = j * mp + q
        top = pl.multiple_of((p // col_parts) * rows + w * piece, 8)
        return pl.ds(top, piece), col_span(p)

    def at(j, q, w):
        return dense.at[spot(j, q, w)]

    rbuf[z] = own

    def pass_grads(k):
        s = (me + dp - 1 - k) % dp
        remote(gbuf.at[s, m], gbuf.at[s, m], g_send.at[k], g_recv.at[s], me, m).wait_recv()
        remote(ibuf.at[s, m], ibuf.at[s, m], i_send.at[k], i_recv.at[s], me, m).wait_recv()
        start_forward(s, gbuf.at[s, m], ibuf.at[s, m])

    loop(dp - 1, pass_grads)

    tables, row_count, width = row_grad.shape
    samples = i_ref.shape[2]
    row_iota = lax.broadcasted_iota(jnp.int32, (row_count, samples), 0) + m * row_count

    def add_source(c):
        s = (me + dp - c) % dp
        for k in range(mp - 1):
            q = (m + 1 + k) % mp
            remote(gbuf.at[s, q], gbuf.at[s, q], gf_send.at[k, s], gf_recv.at[q, s], me, m).wait_recv()
            remote(ibuf.at[s, q], ibuf.at[s, q], if_send.at[k, s], if_recv.at[q, s], me, m).wait_recv()
        for t in range(tables):
            hots = []
            for u in range(mp):
                wanted = ibuf[s, u]
                hot = jnp.zeros((row_count, samples), jnp.float32)
                for n in range(slots):
                    one = wanted[t * slots + n : t * slots + n + 1, :]
                    hot = hot + jnp.where(row_iota == one, 1.0, 0.0)
                hots.append(hot.astype(jnp.bfloat16))
            onehot = jnp.concatenate(hots, axis=1)
            values = gbuf[s, :, t].reshape(mp * samples, width)
            row_grad[t] += jnp.dot(onehot, values, preferred_element_type=jnp.float32)

    early = dp // 2
    loop(early, add_source)

    def wait_sum(k):
        s = (z + 1 + k) % outer
        remote(rbuf.at[s], rbuf.at[s], r_send.at[k], r_recv.at[s], me, m).wait_recv()

    loop(outer - 1, wait_sum)
    total = rbuf[0]
    for w in range(1, outer):
        total = total + rbuf[w]
    dense[spot(i, m, z)] = total

    def z_copy(k):
        w = (z + 1 + k) % outer
        return remote(at(i, m, z), at(i, m, z), z_send.at[k], z_recv.at[z], w * inner + i, m)

    sides = (i + 1 - 2 * (i % 2), (i + 2) % inner)
    across = sides[0] + sides[1] - i
    half = piece // 2

    def x_copy(k, w):
        return remote(at(i, m, w), at(i, m, w), x_send.at[k, w], x_recv.at[k, w], z * inner + sides[k], m)

    def half_at(j, k, w):
        p = j * mp + m
        top = pl.multiple_of((p // col_parts) * rows + w * piece + k * half, 8)
        return dense.at[pl.ds(top, half), col_span(p)]

    def y_copy(k, w):
        here = half_at(sides[k], k, w)
        return remote(here, here, y_send.at[k, w], y_recv.at[k, w], z * inner + sides[1 - k], m)

    def m_copy(k, j, w):
        return remote(at(j, m, w), at(j, m, w), m_send.at[k, j, w], m_recv.at[m, j, w], me, (m + 1 + k) % mp)

    def spread(w):
        if inner > 1:
            for k in range(2):
                x_copy(k, w).start()
        for k in range(mp - 1):
            m_copy(k, i, w).start()

    loop(outer - 1, lambda k: z_copy(k).start())
    spread(z)

    def pass_piece(k):
        w = (z + 1 + k) % outer
        remote(at(i, m, w), at(i, m, w), z_send.at[k], z_recv.at[w], me, m).wait_recv()
        spread(w)

    per = (dp - early) // outer

    def late(k):
        loop(per, lambda c: add_source(early + k * per + c))
        pass_piece(k)

    loop(outer - 1, late)
    done = early + (outer - 1) * per
    loop(dp - done, lambda c: add_source(done + c))

    def pass_side(t):
        w = (z + t) % outer
        for k in range(2):
            j = sides[k]
            remote(at(j, m, w), at(j, m, w), x_send.at[k, w], x_recv.at[k, w], me, m).wait_recv()
            y_copy(k, w).start()
            for n in range(mp - 1):
                m_copy(n, j, w).start()

    def pass_across(t):
        w = (z + t) % outer
        for k in range(2):
            here = half_at(across, k, w)
            remote(here, here, y_send.at[k, w], y_recv.at[k, w], me, m).wait_recv()
        for n in range(mp - 1):
            m_copy(n, across, w).start()

    if inner > 1:
        loop(outer, pass_side)
        loop(outer, pass_across)

    def end_forward(s):
        for k in range(mp - 1):
            for copy in forward(s, k, gbuf.at[s, m], ibuf.at[s, m]):
                copy.wait_send()

    loop(dp, end_forward)

    def end_block(t):
        j, w = t // outer, t % outer
        for k in range(mp - 1):
            q = (m + 1 + k) % mp
            remote(at(j, q, w), at(j, q, w), m_send.at[k, j, w], m_recv.at[q, j, w], me, m).wait_recv()
            m_copy(k, j, w).wait_send()

    loop(inner * outer, end_block)

    def end_a(j):
        for k in range(mp - 1):
            a_pass(k, j, abuf.at[j * mp + m]).wait_send()

    def end_grads(k):
        g_copy(k).wait_send()
        i_copy(k).wait_send()

    loop(inner - 1, lambda k: a_copy(k).wait_send())
    loop(inner, end_a)
    loop(group - 1, lambda k: b_copy(k).wait_send())
    loop(dp - 1, end_grads)

    def end_sum(k):
        r_copy(k).wait_send()
        z_copy(k).wait_send()

    loop(outer - 1, end_sum)

    def end_side(w):
        for k in range(2):
            x_copy(k, w).wait_send()
            y_copy(k, w).wait_send()

    if inner > 1:
        loop(outer, end_side)


def per_device(dp, mp, pooled_grad, bag_lengths, bag_rows, table_rows, row_accum, dense_input, dense_cotangent):
    samples, all_tables, width = pooled_grad.shape
    slots = bag_rows.shape[2]
    tables, row_count = table_rows.shape[0], table_rows.shape[1]
    inner = 4 if dp % 4 == 0 else 1
    outer = dp // inner
    group = inner * mp
    row_parts = 2 if inner % 2 == 0 else 1
    in_width, out_width = dense_input.shape[1], dense_cotangent.shape[1]
    rows, cols = in_width // row_parts, out_width // (group // row_parts)

    slot_iota = jnp.arange(slots, dtype=jnp.int32)
    target = jnp.where(slot_iota[None, None, :] < bag_lengths[..., None], bag_rows, -1)
    target = target.transpose(1, 2, 0).reshape(dp, tables * slots, samples)
    grads = pooled_grad.transpose(1, 0, 2).reshape(dp, tables, samples, width)

    vmem = pl.BlockSpec(memory_space=pltpu.VMEM)
    dma = pltpu.SemaphoreType.DMA
    pairs = max(1, mp - 1)
    dense_grad, row_grad = pl.pallas_call(
        functools.partial(exchange_kernel, dp, mp, inner, row_parts, slots),
        out_shape=(
            jax.ShapeDtypeStruct((in_width, out_width), jnp.float32),
            jax.ShapeDtypeStruct((tables, row_count, width), jnp.float32),
        ),
        in_specs=[vmem] * 4,
        out_specs=(vmem,) * 2,
        scratch_shapes=[
            pltpu.VMEM((dp, mp, tables, samples, width), jnp.bfloat16),
            pltpu.VMEM((dp, mp, tables * slots, samples), jnp.int32),
            pltpu.VMEM((group, samples, rows), jnp.bfloat16),
            pltpu.VMEM((group, samples, cols), jnp.bfloat16),
            pltpu.VMEM((rows, cols), jnp.float32),
            pltpu.VMEM((outer, rows // outer, cols), jnp.float32),
            dma((inner,)), dma((inner,)), dma((pairs, inner)), dma((mp, inner)), dma((group,)), dma((group,)),
            dma((dp,)), dma((dp,)), dma((dp,)), dma((dp,)),
            dma((pairs, dp)), dma((mp, dp)), dma((pairs, dp)), dma((mp, dp)),
            dma((outer,)), dma((outer,)), dma((outer,)), dma((outer,)),
            dma((2, outer)), dma((2, outer)), dma((2, outer)), dma((2, outer)),
            dma((pairs, inner, outer)), dma((mp, inner, outer)),
        ],
        compiler_params=pltpu.CompilerParams(collective_id=0, has_side_effects=True),
        name="exchange",
    )(grads, target, dense_input, dense_cotangent)

    new_accum = row_accum + jnp.mean(row_grad * row_grad, axis=-1)
    new_rows = table_rows - learn_rate * row_grad / jnp.sqrt(new_accum)[..., None]
    return (new_rows, new_accum, dense_grad)


def solution(mesh):
    in_specs = (
        P(("dp", "mp"), None, None),
        P(("dp", "mp"), None),
        P(("dp", "mp"), None, None),
        P("dp", "mp", None),
        P("dp", "mp"),
        P(("dp", "mp"), None),
        P(("dp", "mp"), None),
    )
    out_specs = (P("dp", "mp", None), P("dp", "mp"), P())
    body = functools.partial(per_device, mesh.shape["dp"], mesh.shape["mp"])
    return jax.shard_map(body, mesh=mesh, in_specs=in_specs, out_specs=out_specs, check_vma=False)
```
